1024 devices in a mesh: prompt: 64 (over z, core), sample: 4 (over x), vocab: 4 (over y).
Axes of the slice: x: 4, y: 4, z: 32, core: 2. Of those that a mesh axis runs over, the one named last changes fastest.
Arguments:
- hidden: bfloat16 [4, 768, 3584], P('sample', ('prompt', 'vocab')), may hold values from -170 to 170
- unembed: bfloat16 [152064, 3584], P(('prompt', 'vocab')), may hold values from -1 to 1
- token_ids: int32 [4, 768], P('sample', ('prompt', 'vocab')), may hold values from 0 to 152063, as said below
- old_logp: float32 [4, 768], P('sample', ('prompt', 'vocab')), may hold values from -14 to -11
- ref_logp: float32 [4, 768], P('sample', ('prompt', 'vocab')), may hold values from -14 to -11
- loss_mask: int32 [4, 768], P('sample', ('prompt', 'vocab')), may hold values 0 or 1
- lengths: int32 [64, 4], P('prompt', 'sample'), may hold values from 1 to 12, as said below
- sample_valid: int32 [64, 4], P('prompt', 'sample'), may hold values 0 or 1
- rewards: int32 [64, 4], P('prompt', 'sample'), may hold values from -300 to 300
Outputs:
- token_logp: float32 [4, 768], P('sample', ('prompt', 'vocab'))
- token_loss: float32 [4, 768], P('sample', ('prompt', 'vocab'))
- advantages: float32 [64, 4], P('prompt', 'sample')
- loss: float32 [], replicated
The draws below stay inside these ranges and needn't reach their ends.
Inputs may be any that keep to these rules, and one draw needn't show every extreme that they name: `token_ids`: token ids name vocabulary entries. `lengths`: some response in every draw has length 12.
All inputs are finite; a program needn't handle non-finite values. No bound on the sum of `loss_mask` or of `sample_valid` on one device may be relied on, other than what follows from the above.
Results may differ from the reference program's by a relative error of at most 0.0003.
Values may be sent and summed in bfloat16 or wider, within the bound.
No kernel may reach another device: no remote copies, remote signals or barrier semaphores. Data moves between devices by JAX's collectives and lax.ppermute only.
A program may use at most 64 MiB of HBM per device.

```python
import math
import jax
import jax.numpy as jnp
from jax import lax

D = 3584
VOCAB = 152064
PROMPTS = 64
SAMPLES = 4
LEN = 12
ROWS = 768
N_PROMPT = 64
N_VOCAB = 4


cluster_total = 64


mix_total = 16


def centre_table(key):
    return jnp.clip(jax.random.normal(jax.random.fold_in(key, 13), (cluster_total, D), jnp.float32), -5.5, 5.5)


def weight_row(key, centres, row_index):
    row_key = jax.random.fold_in(jax.random.fold_in(key, 11), row_index)
    first_pick = jax.random.randint(jax.random.fold_in(row_key, 1), (), 0, cluster_total)
    second_pick = jax.random.randint(jax.random.fold_in(row_key, 2), (), 0, cluster_total)
    cluster = jnp.minimum(first_pick, second_pick)
    noise_part = jnp.clip(jax.random.normal(jax.random.fold_in(row_key, 3), (D,), jnp.float32), -5.5, 5.5)
    size_factor = jnp.exp(jax.random.uniform(jax.random.fold_in(row_key, 4), (), jnp.float32, -0.25, 0.25))
    row_value = size_factor * (0.6 * centres[cluster] + 0.8 * noise_part) / math.sqrt(D)
    return jnp.clip(row_value, -1.0, 1.0)


def unembed_rows(key, indices):
    centres = centre_table(key)
    return jax.vmap(lambda row_index: weight_row(key, centres, row_index))(indices)


def label_table(key):
    return jax.random.randint(jax.random.fold_in(key, 23), (SAMPLES, ROWS), 0, VOCAB, dtype=jnp.int32)


def draw_unembed(key, part):
    return unembed_rows(key, jnp.arange(VOCAB, dtype=jnp.int32)).astype(jnp.bfloat16)


def draw_token_ids(key, part):
    return label_table(key)


def draw_hidden(key, part):
    flat_count = SAMPLES * ROWS
    noise_part = jnp.clip(jax.random.normal(jax.random.fold_in(key, 31), (flat_count, D), jnp.float32), -6.0, 6.0)
    picks = jax.random.randint(jax.random.fold_in(key, 43), (flat_count, mix_total), 0, VOCAB, dtype=jnp.int32)
    mix_weights = jax.random.uniform(jax.random.fold_in(key, 47), (flat_count, mix_total), jnp.float32, 3.0, 7.0)
    noise_scale = 0.5
    centres = centre_table(key)

    def mixture(item):
        row_picks, row_weights = item
        chosen_rows = jax.vmap(lambda row_index: weight_row(key, centres, row_index))(row_picks)
        return jnp.sum(row_weights[:, None] * chosen_rows, axis=0)
    mixed = lax.map(mixture, (picks, mix_weights))
    values = mixed + noise_scale * noise_part
    values = jnp.clip(values, -170.0, 170.0)
    return values.reshape(SAMPLES, ROWS, D).astype(jnp.bfloat16)


def draw_lengths(key, part):
    col_caps = jax.random.randint(jax.random.fold_in(key, 53), (SAMPLES,), 1, LEN + 1)
    raw_draw = jax.random.randint(jax.random.fold_in(key, 59), (PROMPTS, SAMPLES), 0, LEN)
    length_draw = 1 + raw_draw * col_caps[None, :] // LEN
    longest = jax.random.randint(jax.random.fold_in(key, 61), (), 0, SAMPLES)
    column = lax.broadcasted_iota(jnp.int32, (PROMPTS, SAMPLES), 1)
    row_line = lax.broadcasted_iota(jnp.int32, (PROMPTS, SAMPLES), 0)
    return jnp.where((column == longest) & (row_line == 0), LEN, length_draw).astype(jnp.int32)


def place_ends(drawn, key, smallest, largest):
    longest = drawn.shape.index(max(drawn.shape))
    spots = []
    for shift in (0, 1):
        where = [jax.random.randint(jax.random.fold_in(key, axis), (), 0, length) for axis, length in enumerate(drawn.shape)]
        where[longest] = (where[longest] + shift) % drawn.shape[longest]
        spots.append(tuple(where))
    return drawn.at[spots[0]].set(smallest).at[spots[1]].set(largest)


def level_of(own_key, dims, pieces, low, largest):
    factor_of = 1.0
    for axis_at, shards_of in pieces:
        steps = jax.random.uniform(jax.random.fold_in(jax.random.fold_in(own_key, 6), axis_at), (shards_of,), jnp.float32, low / len(pieces), largest / len(pieces))
        factor_of = factor_of * jnp.repeat(jnp.exp(steps), dims[axis_at] // shards_of).reshape((-1,) + (1,) * (len(dims) - 1 - axis_at))
    return factor_of


def setup_inputs(seed: int = 0) -> dict:
    arg_keys = jax.random.split(jax.random.key(seed), 10)
    hidden = draw_hidden(jax.random.fold_in(arg_keys[9], 71), 0)
    unembed = draw_unembed(jax.random.fold_in(arg_keys[9], 71), 0)
    token_ids = draw_token_ids(jax.random.fold_in(arg_keys[9], 71), 0)
    old_logp = jnp.clip(-14.0 + 3.0 * jax.random.uniform(arg_keys[3], (SAMPLES, ROWS), jnp.float32) ** level_of(arg_keys[3], (SAMPLES, ROWS), ((0, 4), (1, 256)), -0.2, 0.2), -14.0, -11.0)
    ref_logp = jnp.clip(-14.0 + 3.0 * jax.random.uniform(arg_keys[4], (SAMPLES, ROWS), jnp.float32) ** level_of(arg_keys[4], (SAMPLES, ROWS), ((0, 4), (1, 256)), -0.2, 0.2), -14.0, -11.0)
    loss_mask = place_ends((jax.random.randint(arg_keys[5], (SAMPLES, ROWS), 0, 8) < 7).astype(jnp.int32), jax.random.fold_in(arg_keys[5], 1), 0, 1)
    lengths = draw_lengths(jax.random.fold_in(arg_keys[9], 71), 0)
    sample_valid = place_ends((jax.random.randint(arg_keys[7], (PROMPTS, SAMPLES), 0, 8) < 7).astype(jnp.int32), jax.random.fold_in(arg_keys[7], 1), 0, 1)
    rewards = place_ends(jax.random.randint(arg_keys[8], (PROMPTS, SAMPLES), -300, 301), jax.random.fold_in(arg_keys[8], 1), -300, 300).astype(jnp.int32)
    return {"hidden": hidden, "unembed": unembed, "token_ids": token_ids, "old_logp": old_logp, "ref_logp": ref_logp, "loss_mask": loss_mask, "lengths": lengths, "sample_valid": sample_valid, "rewards": rewards}


clip_low = 0.8
clip_high = 1.2
dual_clip = 3.0
kl_weight = 0.04
reward_unit = 0.01
std_floor = 0.5
low_fill = -1e+30

def reference(hidden, unembed, token_ids, old_logp, ref_logp, loss_mask, lengths, sample_valid, rewards):
    samples, row_count, width = hidden.shape
    flat_count = samples * row_count
    flat_hidden = hidden.reshape(flat_count, width)
    flat_ids = token_ids.reshape(flat_count)
    shard_count = N_PROMPT * N_VOCAB
    shard_rows = unembed.shape[0] // shard_count
    shard_blocks = unembed.reshape(shard_count, shard_rows, width)

    def scan_step(totals, shard_item):
        run_peak, run_total, run_target = totals
        shard_block, shard_idx = shard_item
        logits = jnp.dot(flat_hidden, shard_block.T, preferred_element_type=jnp.float32)
        new_peak = jnp.maximum(run_peak, lax.optimization_barrier(jnp.max(logits, axis=1)))
        run_total = run_total * jnp.exp(run_peak - new_peak) + lax.optimization_barrier(jnp.sum(jnp.exp(logits - new_peak[:, None]), axis=1))
        column = shard_idx * shard_rows + lax.broadcasted_iota(jnp.int32, logits.shape, 1)
        run_target = run_target + lax.optimization_barrier(jnp.sum(jnp.where(column == flat_ids[:, None], logits, 0.0), axis=1))
        return ((new_peak, run_total, run_target), None)
    start_fill = (jnp.full((flat_count,), low_fill, jnp.float32), jnp.zeros((flat_count,), jnp.float32), jnp.zeros((flat_count,), jnp.float32))
    (run_peak, run_total, run_target), unused = lax.scan(scan_step, start_fill, (shard_blocks, jnp.arange(shard_count, dtype=jnp.int32)))
    raw_logp = (run_target - (run_peak + jnp.log(run_total))).reshape(samples, row_count)
    positions = lax.broadcasted_iota(jnp.int32, (samples, row_count), 1) % LEN
    length_rows = jnp.repeat(lengths.T, LEN, axis=1)
    valid_rows = jnp.repeat(sample_valid.T, LEN, axis=1)
    live_rows = (loss_mask == 1) & (positions < length_rows) & (valid_rows == 1)
    token_logp = jnp.where(live_rows, raw_logp, 0.0)
    valid_f = sample_valid.astype(jnp.float32)
    scores = rewards.astype(jnp.float32) * reward_unit
    group_count = lax.optimization_barrier(jnp.sum(valid_f, axis=1))
    first_moment = lax.optimization_barrier(jnp.sum(valid_f * scores, axis=1))
    second_moment = lax.optimization_barrier(jnp.sum(valid_f * scores * scores, axis=1))
    safe_count = jnp.maximum(group_count, 1.0)
    group_mean = first_moment / safe_count
    spread = jnp.sqrt(jnp.maximum(second_moment / safe_count - group_mean * group_mean, 0.0))
    advantages = valid_f * (scores - group_mean[:, None]) / jnp.maximum(spread, std_floor)[:, None]
    adv_rows = jnp.repeat(advantages.T, LEN, axis=1)
    prob_ratio = jnp.exp(raw_logp - old_logp)
    gain_side = adv_rows * jnp.minimum(prob_ratio, clip_high)
    loss_side = jnp.maximum(adv_rows * jnp.maximum(prob_ratio, clip_low), dual_clip * adv_rows)
    objective = jnp.where(adv_rows >= 0.0, gain_side, loss_side)
    log_gap = ref_logp - raw_logp
    kl_term = jnp.exp(log_gap) - log_gap - 1.0
    token_loss = jnp.where(live_rows, kl_weight * kl_term - objective, 0.0)
    live_total = jnp.sum(live_rows.astype(jnp.float32))
    loss = jnp.sum(token_loss) / jnp.maximum(live_total, 1.0)
    return (token_logp, token_loss, advantages, loss)
```

```python
import jax
import jax.numpy as jnp
from jax import lax
from jax.experimental import pallas as pl
from jax.experimental.pallas import tpu as pltpu
from jax.sharding import Mesh
from jax.sharding import PartitionSpec as P

FAR = 8
NEAR = 4
ROW = ("zh", "zn", "c", "y")
PROMPT = ("zh", "zn", "c")
Z = ("zh", "zn")
PLANE = ("c", "x", "y")

clip_low = 0.8
clip_high = 1.2
dual_clip = 3.0
kl_weight = 0.04
reward_unit = 0.01
std_floor = 0.5


def from_everyone(array, axis):
    devices = lax.axis_size(axis)
    return lax.all_to_all(
        jnp.broadcast_to(array[None], (devices, *array.shape)), axis, 0, 0, tiled=True
    )


def stats_kernel(x_ref, w_ref, ids_ref, out_ref):
    groups, _, per = out_ref.shape
    logits = lax.dot_general(
        w_ref[...], x_ref[...], (((1,), (1,)), ((), ())), preferred_element_type=jnp.float32
    )
    peak = jnp.max(logits, axis=0, keepdims=True)
    total = jnp.sum(jnp.exp(logits - peak), axis=0, keepdims=True)
    line = lax.broadcasted_iota(jnp.int32, logits.shape, 0)
    target = jnp.sum(jnp.where(line == ids_ref[...], logits, 0.0), axis=0, keepdims=True)
    for g in range(groups):
        out_ref[g, 0:1, :] = peak[:, g * per : (g + 1) * per]
        out_ref[g, 1:2, :] = total[:, g * per : (g + 1) * per]
        out_ref[g, 2:3, :] = target[:, g * per : (g + 1) * per]


def shard_stats(rows, weight, local_ids, groups):
    count, width = rows.shape
    vocab = weight.shape[0]
    return pl.pallas_call(
        stats_kernel,
        out_shape=jax.ShapeDtypeStruct((groups, 3, count // groups), jnp.float32),
        cost_estimate=pl.CostEstimate(
            flops=2 * count * width * vocab,
            bytes_accessed=2 * width * (count + vocab),
            transcendentals=count * vocab,
        ),
        name="shard_stats",
    )(rows, weight, local_ids)


def merged(stats):
    peak = jnp.max(stats[:, 0], axis=0)
    total = jnp.sum(stats[:, 1] * jnp.exp(stats[:, 0] - peak), axis=0)
    target = jnp.sum(stats[:, 2], axis=0)
    return jnp.stack([peak, total, target])


def local(
    hidden, unembed, token_ids, old_logp, ref_logp, loss_mask, lengths, sample_valid, rewards
):
    _, local_rows, width = hidden.shape
    vocab_rows = unembed.shape[0]
    n_y = lax.axis_size("y")
    n_z = lax.axis_size(Z)
    column_rows = n_z * local_rows
    core = lax.axis_index("c")

    far = from_everyone(hidden.reshape(local_rows * width // 128, 128), "zh")
    near = from_everyone(far, "zn")
    rows = (
        near.reshape(NEAR, FAR, local_rows, width)
        .transpose(1, 0, 2, 3)
        .reshape(column_rows, width)
    )
    own = from_everyone(rows, "y").reshape(n_y * column_rows, width)
    other = lax.ppermute(own, "c", [(0, 1), (1, 0)])

    positions = lax.axis_index("y") * local_rows + lax.broadcasted_iota(
        jnp.int32, (1, local_rows), 1
    )
    live_rows = (loss_mask == 1) & (positions < lengths.T) & (sample_valid.T == 1)
    valid_f = sample_valid.astype(jnp.float32)
    scores = rewards.astype(jnp.float32) * reward_unit
    moments = from_everyone(
        jnp.concatenate([valid_f, valid_f * scores, valid_f * scores * scores], axis=1), "x"
    )
    group_count, first_moment, second_moment = jnp.split(jnp.sum(moments, axis=0), 3, axis=1)
    safe_count = jnp.maximum(group_count, 1.0)
    group_mean = first_moment / safe_count
    spread = jnp.sqrt(jnp.maximum(second_moment / safe_count - group_mean * group_mean, 0.0))
    advantages = valid_f * (scores - group_mean) / jnp.maximum(spread, std_floor)

    side = jnp.concatenate(
        [
            token_ids.astype(jnp.float32),
            old_logp,
            ref_logp,
            live_rows.astype(jnp.float32),
            jnp.broadcast_to(advantages, (1, local_rows)),
        ]
    )
    side = from_everyone(side, Z).transpose(1, 0, 2).reshape(5, column_rows)
    vocab_start = lax.axis_index(ROW) * vocab_rows
    all_ids = from_everyone(side[0:1].astype(jnp.int32), ("c", "y")) - vocab_start
    all_ids = all_ids.reshape(2, n_y * column_rows)
    own_ids = lax.dynamic_slice_in_dim(all_ids, core, 1, 0)
    other_ids = lax.dynamic_slice_in_dim(all_ids, 1 - core, 1, 0)

    own_stats = shard_stats(own, unembed, own_ids, n_y)
    other_stats = shard_stats(other, unembed, other_ids, n_y)
    low = jnp.where(core == 0, own_stats, other_stats)
    high = jnp.where(core == 0, other_stats, own_stats)
    plane = lax.all_to_all(jnp.concatenate([low, high]), ("c", "y"), 0, 0, tiled=True)
    total = merged(from_everyone(merged(plane), Z))
    raw_logp = total[2:3] - (total[0:1] + jnp.log(total[1:2]))

    live = side[3:4] > 0.5
    adv_rows = side[4:5]
    token_logp = jnp.where(live, raw_logp, 0.0)
    prob_ratio = jnp.exp(raw_logp - side[1:2])
    gain_side = adv_rows * jnp.minimum(prob_ratio, clip_high)
    loss_side = jnp.maximum(adv_rows * jnp.maximum(prob_ratio, clip_low), dual_clip * adv_rows)
    objective = jnp.where(adv_rows >= 0.0, gain_side, loss_side)
    log_gap = side[2:3] - raw_logp
    kl_term = jnp.exp(log_gap) - log_gap - 1.0
    token_loss = jnp.where(live, kl_weight * kl_term - objective, 0.0)
    sums = jnp.stack([jnp.sum(token_loss), jnp.sum(side[3:4])])
    sums = jnp.sum(from_everyone(sums, PLANE), axis=0)
    loss = sums[0] / jnp.maximum(sums[1], 1.0)
    start = lax.axis_index(Z) * local_rows
    return (
        lax.dynamic_slice_in_dim(token_logp, start, local_rows, 1),
        lax.dynamic_slice_in_dim(token_loss, start, local_rows, 1),
        advantages,
        loss,
    )


def solution(mesh):
    split = Mesh(
        mesh.devices.reshape(FAR, NEAR, 2, mesh.shape["sample"], mesh.shape["vocab"]),
        ("zh", "zn", "c", "x", "y"),
    )
    in_specs = (
        P("x", ROW, None),
        P(ROW, None),
        P("x", ROW),
        P("x", ROW),
        P("x", ROW),
        P("x", ROW),
        P(PROMPT, "x"),
        P(PROMPT, "x"),
        P(PROMPT, "x"),
    )
    out_specs = (P("x", ROW), P("x", ROW), P(PROMPT, "x"), P())
    return jax.shard_map(local, mesh=split, in_specs=in_specs, out_specs=out_specs, check_vma=False)
```

```python
import jax
import jax.numpy as jnp
from jax import lax
from jax.experimental import pallas as pl
from jax.experimental.pallas import tpu as pltpu
from jax.sharding import Mesh
from jax.sharding import PartitionSpec as P


ROW = ("z", "c", "y")
PROMPT = ("z", "c")
PLANE = ("c", "x", "y")
LANES = 128
KERNEL_VMEM = 24 * 2**20

clip_low = 0.8
clip_high = 1.2
dual_clip = 3.0
kl_weight = 0.04
reward_unit = 0.01
std_floor = 0.5


def from_everyone(array, axis):
    devices = lax.axis_size(axis)
    return lax.all_to_all(
        jnp.broadcast_to(array[None], (devices, *array.shape)), axis, 0, 0, tiled=True
    )


def split_exact(values):
    pieces = []
    for _ in range(3):
        piece = lax.reduce_precision(values, 8, 7)
        pieces.append(piece.astype(jnp.bfloat16))
        values = values - piece
    return pieces


def stats_kernel(start_ref, x_ref, own_ref, other_ref, out_ref):
    groups, _, per = out_ref.shape
    vocab, width = own_ref.shape
    rows = x_ref[:, :width]
    side = x_ref[:, width:]
    pick = (lax.broadcasted_iota(jnp.int32, (8, LANES), 1) < 3).astype(jnp.bfloat16)
    contract = (((1,), (1,)), ((), ()))
    ids = lax.dot_general(pick, side, contract, preferred_element_type=jnp.float32)
    ids = ids[0:1].astype(jnp.int32)
    line = lax.broadcasted_iota(jnp.int32, (vocab, rows.shape[0]), 0)
    parts = []
    for half, w_ref in enumerate((own_ref, other_ref)):
        logits = lax.dot_general(w_ref[...], rows, contract, preferred_element_type=jnp.float32)
        peak = jnp.max(logits, axis=0, keepdims=True)
        total = jnp.sum(jnp.exp(logits - peak), axis=0, keepdims=True)
        hit = line == ids - start_ref[half]
        parts.append((peak, total, jnp.sum(jnp.where(hit, logits, 0.0), axis=0, keepdims=True)))
    (peak_a, total_a, target_a), (peak_b, total_b, target_b) = parts
    peak = jnp.maximum(peak_a, peak_b)
    total = total_a * jnp.exp(peak_a - peak) + total_b * jnp.exp(peak_b - peak)
    lse = peak + jnp.log(total)
    target = target_a + target_b
    for g in range(groups):
        out_ref[g, 0:1, :] = lse[:, g * per : (g + 1) * per]
        out_ref[g, 1:2, :] = target[:, g * per : (g + 1) * per]


def shard_stats(rows, own, other, starts, groups):
    count = rows.shape[0]
    vocab, width = own.shape
    return pl.pallas_call(
        stats_kernel,
        in_specs=[
            pl.BlockSpec(memory_space=pltpu.SMEM),
            pl.BlockSpec(memory_space=pltpu.VMEM),
            pl.BlockSpec(memory_space=pltpu.VMEM),
            pl.BlockSpec(memory_space=pltpu.VMEM),
        ],
        out_specs=pl.BlockSpec(memory_space=pltpu.VMEM),
        out_shape=jax.ShapeDtypeStruct((groups, 2, count // groups), jnp.float32),
        cost_estimate=pl.CostEstimate(
            flops=4 * count * width * vocab,
            bytes_accessed=2 * width * (count + 2 * vocab),
            transcendentals=2 * count * vocab,
        ),
        compiler_params=pltpu.CompilerParams(vmem_limit_bytes=KERNEL_VMEM),
        name="shard_stats",
    )(starts, rows, own, other)


def merged(lse):
    peak = jnp.max(lse, axis=0)
    return peak + jnp.log(jnp.sum(jnp.exp(lse - peak), axis=0))


def group_advantages(sums, valid_f, scores):
    group_count, first_moment, second_moment = (sums[i : i + 1] for i in range(3))
    safe_count = jnp.maximum(group_count, 1.0)
    group_mean = first_moment / safe_count
    spread = jnp.sqrt(jnp.maximum(second_moment / safe_count - group_mean * group_mean, 0.0))
    return valid_f * (scores - group_mean) / jnp.maximum(spread, std_floor)


def local(
    hidden, unembed, token_ids, old_logp, ref_logp, loss_mask, lengths, sample_valid, rewards
):
    _, local_rows, width = hidden.shape
    vocab_rows = unembed.shape[0]
    n_x = lax.axis_size("x")
    n_y = lax.axis_size("y")
    n_z = lax.axis_size("z")
    column_rows = n_z * local_rows
    core = lax.axis_index("c")

    positions = lax.axis_index("y") * local_rows + lax.broadcasted_iota(
        jnp.int32, (1, local_rows), 1
    )
    live_rows = (loss_mask == 1) & (positions < lengths.T) & (sample_valid.T == 1)
    fields = jnp.concatenate(
        [
            token_ids.astype(jnp.float32),
            old_logp,
            ref_logp,
            live_rows.astype(jnp.float32),
            jnp.broadcast_to(sample_valid.astype(jnp.float32), (1, local_rows)),
            jnp.broadcast_to(rewards.astype(jnp.float32), (1, local_rows)),
        ]
    )
    n_fields = fields.shape[0]
    pieces = jnp.stack(split_exact(fields.T), axis=2).reshape(local_rows, 3 * n_fields)
    pieces = jnp.pad(pieces, ((0, 0), (0, LANES - 3 * n_fields)))
    full = width + LANES
    chunk = jnp.concatenate([hidden[0], pieces], axis=1).reshape(local_rows * full // LANES, LANES)
    tall = -(-chunk.shape[0] // 8) * 8
    column = lax.all_gather(jnp.pad(chunk, ((0, tall - chunk.shape[0]), (0, 0))), "z", axis=0)
    rows = column[:, : chunk.shape[0]].reshape(column_rows, full)

    other_unembed = lax.ppermute(unembed, "c", [(0, 1), (1, 0)])
    gathered = from_everyone(rows, "y").reshape(n_y * column_rows, full)

    side = rows[:, width : width + 3 * n_fields].astype(jnp.float32).T
    side = side.reshape(n_fields, 3, column_rows)
    side = side[:, 0] + side[:, 1] + side[:, 2]
    old_rows, ref_rows, live_float, valid_f, reward_rows = (side[i : i + 1] for i in range(1, 6))
    scores = reward_rows * reward_unit
    moments = jnp.concatenate([valid_f, valid_f * scores, valid_f * scores * scores])
    terms = [moments]
    for d in range(1, n_x):
        ring = [(i, (i + d) % n_x) for i in range(n_x)]
        terms.append(lax.ppermute(moments, "x", ring))
    adv_rows = group_advantages(sum(terms), valid_f, scores)
    z = lax.axis_index("z")
    shards = jnp.stack([(z * 2 + core) * n_y, (z * 2 + 1 - core) * n_y]) + lax.axis_index("y")
    stats = shard_stats(gathered, unembed, other_unembed, shards * vocab_rows, n_y)
    plane = lax.all_to_all(stats, "y", 0, 0, tiled=True)
    plane = jnp.concatenate([merged(plane[:, 0:1]), jnp.sum(plane[:, 1:2], axis=0)])
    back = from_everyone(plane, "z")
    raw_logp = jnp.sum(back[:, 1:2], axis=0) - merged(back[:, 0:1])

    live = live_float > 0.5
    token_logp = jnp.where(live, raw_logp, 0.0)
    prob_ratio = jnp.exp(raw_logp - old_rows)
    gain_side = adv_rows * jnp.minimum(prob_ratio, clip_high)
    loss_side = jnp.maximum(adv_rows * jnp.maximum(prob_ratio, clip_low), dual_clip * adv_rows)
    objective = jnp.where(adv_rows >= 0.0, gain_side, loss_side)
    log_gap = ref_rows - raw_logp
    kl_term = jnp.exp(log_gap) - log_gap - 1.0
    token_loss = jnp.where(live, kl_weight * kl_term - objective, 0.0)
    totals = jnp.stack([jnp.sum(token_loss), jnp.sum(live_float)])
    totals = jnp.sum(from_everyone(totals, PLANE), axis=0)
    loss = totals[0] / jnp.maximum(totals[1], 1.0)
    first = z * local_rows
    return (
        lax.dynamic_slice_in_dim(token_logp, first, local_rows, 1),
        lax.dynamic_slice_in_dim(token_loss, first, local_rows, 1),
        lax.dynamic_slice_in_dim(adv_rows, first, 1, 1),
        loss,
    )


def solution(mesh):
    split = Mesh(
        mesh.devices.reshape(
            mesh.shape["prompt"] // 2, 2, mesh.shape["sample"], mesh.shape["vocab"]
        ),
        ("z", "c", "x", "y"),
    )
    in_specs = (
        P("x", ROW, None),
        P(ROW, None),
        P("x", ROW),
        P("x", ROW),
        P("x", ROW),
        P("x", ROW),
        P(PROMPT, "x"),
        P(PROMPT, "x"),
        P(PROMPT, "x"),
    )
    out_specs = (P("x", ROW), P("x", ROW), P(PROMPT, "x"), P())
    return jax.shard_map(local, mesh=split, in_specs=in_specs, out_specs=out_specs, check_vma=False)
```

```python
import jax
import jax.numpy as jnp
from jax import lax
from jax.experimental import pallas as pl
from jax.experimental.pallas import tpu as pltpu
from jax.sharding import Mesh
from jax.sharding import PartitionSpec as P


Z = ("zh", "zl")
ROW = ("zh", "zl", "c", "y")
PROMPT = ("zh", "zl", "c")
PLANE = ("c", "x", "y")
LANES = 128
FIELDS = 6
FULL_VMEM = 60 * 1024 * 2**10
KERNEL_VMEM = 48 * 2**20
SMALL_VMEM = 4 * 2**20

clip_low = 0.8
clip_high = 1.2
dual_clip = 3.0
kl_weight = 0.04
reward_unit = 0.01
std_floor = 0.5


def from_everyone(array, axis):
    devices = lax.axis_size(axis)
    return lax.all_to_all(
        jnp.broadcast_to(array[None], (devices, *array.shape)), axis, 0, 0, tiled=True
    )


def prep_kernel(y_ref, *refs):
    smalls, hidden_ref, out_ref, tall_ref = refs[:7], refs[7], refs[8], refs[9]
    landed, sems = refs[10:17], refs[17]
    copies = [
        pltpu.make_async_copy(src, dst, sems.at[i])
        for i, (src, dst) in enumerate(zip(smalls, landed))
    ]
    for copy in copies:
        copy.start()
    for copy in copies:
        copy.wait()
    ids_ref, old_ref, ref_ref, mask_ref, len_ref, valid_ref, reward_ref = landed
    local_rows, width = hidden_ref.shape[1:]
    blocks = width // LANES
    lane = lax.broadcasted_iota(jnp.int32, (local_rows, LANES), 1)
    line = lax.broadcasted_iota(jnp.int32, (local_rows, LANES), 0)
    field = lane // 3
    values = jnp.zeros((local_rows, LANES), jnp.float32)
    for r in range(local_rows):
        position = y_ref[0] * local_rows + r
        live = (mask_ref[0, r] == 1) & (position < len_ref[0]) & (valid_ref[0] == 1)
        whole = jnp.where(
            field == 0,
            ids_ref[0, r],
            jnp.where(
                field == 3,
                live.astype(jnp.int32),
                jnp.where(
                    field == 4, valid_ref[0], jnp.where(field == 5, reward_ref[0], 0)
                ),
            ),
        ).astype(jnp.float32)
        row = jnp.where(
            field == 1, old_ref[0, r], jnp.where(field == 2, ref_ref[0, r], whole)
        )
        values = jnp.where(line == r, row, values)
    first = values.astype(jnp.bfloat16).astype(jnp.float32)
    rest = values - first
    second = rest.astype(jnp.bfloat16).astype(jnp.float32)
    piece = lane - 3 * field
    side = jnp.where(piece == 0, first, jnp.where(piece == 1, second, rest - second))
    tall_ref[...] = jnp.zeros(tall_ref.shape, jnp.float32)
    for r in range(local_rows):
        at = r * (blocks + 1)
        for j in range(blocks):
            part = hidden_ref[0, r : r + 1, j * LANES : (j + 1) * LANES]
            tall_ref[at + j : at + j + 1, :] = part.astype(jnp.float32)
        tall_ref[at + blocks : at + blocks + 1, :] = side[r : r + 1, :]
    out_ref[...] = tall_ref[...].astype(jnp.bfloat16)


def prepared(y, smalls, hidden):
    _, local_rows, width = hidden.shape
    tall = -(-local_rows * (width // LANES + 1) // 8) * 8
    vmem = pl.BlockSpec(memory_space=pltpu.VMEM)
    return pl.pallas_call(
        prep_kernel,
        in_specs=[pl.BlockSpec(memory_space=pltpu.SMEM)]
        + [pl.BlockSpec(memory_space=pltpu.HBM)] * len(smalls)
        + [vmem],
        out_specs=vmem,
        out_shape=jax.ShapeDtypeStruct((tall, LANES), jnp.bfloat16),
        scratch_shapes=[
            pltpu.VMEM((tall, LANES), jnp.float32),
            *(pltpu.SMEM(small.shape, small.dtype) for small in smalls),
            pltpu.SemaphoreType.DMA((len(smalls),)),
        ],
        compiler_params=pltpu.CompilerParams(vmem_limit_bytes=FULL_VMEM),
        name="prep",
    )(y, *smalls, hidden)


def tail_kernel(back_ref, side_ref, adv_ref, logp_ref, loss_ref, totals_ref):
    lse = back_ref[:, 0, :]
    peak = jnp.max(lse, axis=0, keepdims=True)
    total = jnp.sum(jnp.exp(lse - peak), axis=0, keepdims=True)
    target = jnp.sum(back_ref[:, 1, :], axis=0, keepdims=True)
    raw_logp = target - (peak + jnp.log(total))
    live_float = side_ref[3:4, :]
    live = live_float > 0.5
    adv_rows = adv_ref[...]
    prob_ratio = jnp.exp(raw_logp - side_ref[1:2, :])
    gain_side = adv_rows * jnp.minimum(prob_ratio, clip_high)
    loss_side = jnp.maximum(adv_rows * jnp.maximum(prob_ratio, clip_low), dual_clip * adv_rows)
    objective = jnp.where(adv_rows >= 0.0, gain_side, loss_side)
    log_gap = side_ref[2:3, :] - raw_logp
    kl_term = jnp.exp(log_gap) - log_gap - 1.0
    token_loss = jnp.where(live, kl_weight * kl_term - objective, 0.0)
    logp_ref[...] = jnp.where(live, raw_logp, 0.0)
    loss_ref[...] = token_loss
    lane = lax.broadcasted_iota(jnp.int32, totals_ref.shape, 2)
    totals_ref[...] = jnp.where(
        lane == 0, jnp.sum(token_loss), jnp.where(lane == 1, jnp.sum(live_float), 0.0)
    )


def finished(back, side, adv_rows, devices):
    row = jax.ShapeDtypeStruct(adv_rows.shape, jnp.float32)
    vmem = pl.BlockSpec(memory_space=pltpu.VMEM)
    return pl.pallas_call(
        tail_kernel,
        in_specs=[vmem] * 3,
        out_specs=[vmem] * 3,
        out_shape=[row, row, jax.ShapeDtypeStruct((devices, 1, LANES), jnp.float32)],
        compiler_params=pltpu.CompilerParams(vmem_limit_bytes=SMALL_VMEM),
        name="tail",
    )(back, side, adv_rows)


def stats_kernel(start_ref, x_ref, own_ref, other_ref, out_ref, weights_ref, sems):
    groups, _, per = out_ref.shape
    vocab, width = own_ref.shape
    half = 8 * LANES
    copies = [
        pltpu.make_async_copy(own_ref.at[:, :half], weights_ref.at[0, :, :half], sems.at[0]),
        pltpu.make_async_copy(own_ref.at[:, half:], weights_ref.at[0, :, half:], sems.at[1]),
        pltpu.make_async_copy(other_ref, weights_ref.at[1], sems.at[2]),
    ]
    for copy in copies:
        copy.start()
    contract = (((1,), (1,)), ((), ()))

    def product(left, right):
        return lax.dot_general(left, right, contract, preferred_element_type=jnp.float32)

    pick = (lax.broadcasted_iota(jnp.int32, (8, LANES), 1) < 3).astype(jnp.bfloat16)
    ids = product(pick, x_ref[:, width:])[0:1].astype(jnp.int32)
    line = lax.broadcasted_iota(jnp.int32, (vocab, x_ref.shape[0]), 0)

    def stats(logits, start):
        peak = jnp.max(logits, axis=0, keepdims=True)
        total = jnp.sum(jnp.exp(logits - peak), axis=0, keepdims=True)
        hit = line == ids - start
        return peak, total, jnp.sum(jnp.where(hit, logits, 0.0), axis=0, keepdims=True)

    copies[0].wait()
    logits = product(weights_ref[0, :, :half], x_ref[:, :half])
    copies[1].wait()
    logits += product(weights_ref[0, :, half:], x_ref[:, half:width])
    peak_a, total_a, target_a = stats(logits, start_ref[0])
    copies[2].wait()
    logits = product(weights_ref[1], x_ref[:, :width])
    peak_b, total_b, target_b = stats(logits, start_ref[1])
    peak = jnp.maximum(peak_a, peak_b)
    total = total_a * jnp.exp(peak_a - peak) + total_b * jnp.exp(peak_b - peak)
    lse = peak + jnp.log(total)
    target = target_a + target_b
    for g in range(groups):
        out_ref[g, 0:1, :] = lse[:, g * per : (g + 1) * per]
        out_ref[g, 1:2, :] = target[:, g * per : (g + 1) * per]


def shard_stats(rows, own, other, starts, groups):
    count = rows.shape[0]
    vocab, width = own.shape
    return pl.pallas_call(
        stats_kernel,
        in_specs=[
            pl.BlockSpec(memory_space=pltpu.SMEM),
            pl.BlockSpec(memory_space=pltpu.VMEM),
            pl.BlockSpec(memory_space=pltpu.HBM),
            pl.BlockSpec(memory_space=pltpu.HBM),
        ],
        out_specs=pl.BlockSpec(memory_space=pltpu.VMEM),
        out_shape=jax.ShapeDtypeStruct((groups, 2, count // groups), jnp.float32),
        scratch_shapes=[
            pltpu.VMEM((2, vocab, width), jnp.bfloat16),
            pltpu.SemaphoreType.DMA((3,)),
        ],
        cost_estimate=pl.CostEstimate(
            flops=4 * count * width * vocab,
            bytes_accessed=2 * width * (count + 2 * vocab),
            transcendentals=2 * count * vocab,
        ),
        compiler_params=pltpu.CompilerParams(vmem_limit_bytes=KERNEL_VMEM),
        name="shard_stats",
    )(starts, rows, own, other)


def merged(lse):
    peak = jnp.max(lse, axis=0)
    return peak + jnp.log(jnp.sum(jnp.exp(lse - peak), axis=0))


def group_advantages(sums, valid_f, scores):
    group_count, first_moment, second_moment = (sums[i : i + 1] for i in range(3))
    safe_count = jnp.maximum(group_count, 1.0)
    group_mean = first_moment / safe_count
    spread = jnp.sqrt(jnp.maximum(second_moment / safe_count - group_mean * group_mean, 0.0))
    return valid_f * (scores - group_mean) / jnp.maximum(spread, std_floor)


def local(
    hidden, unembed, token_ids, old_logp, ref_logp, loss_mask, lengths, sample_valid, rewards
):
    _, local_rows, width = hidden.shape
    vocab_rows = unembed.shape[0]
    n_x = lax.axis_size("x")
    n_y = lax.axis_size("y")
    n_z = lax.axis_size(Z)
    column_rows = n_z * local_rows
    core = lax.axis_index("c")

    full = width + LANES
    y = lax.axis_index("y")
    singles = (lengths.reshape(1), sample_valid.reshape(1), rewards.reshape(1))
    smalls = (token_ids, old_logp, ref_logp, loss_mask, *singles)
    chunk = prepared(y.reshape(1), smalls, hidden)
    column = lax.all_gather(lax.all_gather(chunk, "zh", axis=0), "zl", axis=0)
    column = column.reshape(n_z, *chunk.shape)
    rows = column[:, : local_rows * full // LANES].reshape(column_rows, full)

    other_unembed = lax.ppermute(unembed, "c", [(0, 1), (1, 0)])
    gathered = from_everyone(rows, "y").reshape(n_y * column_rows, full)

    side = rows[:, width : width + 3 * FIELDS].astype(jnp.float32).T
    side = side.reshape(FIELDS, 3, column_rows)
    side = side[:, 0] + side[:, 1] + side[:, 2]
    valid_f = side[4:5]
    scores = side[5:6] * reward_unit
    moments = jnp.concatenate([valid_f, valid_f * scores, valid_f * scores * scores])
    terms = [moments]
    for d in range(1, n_x):
        ring = [(i, (i + d) % n_x) for i in range(n_x)]
        terms.append(lax.ppermute(moments, "x", ring))
    adv_rows = group_advantages(sum(terms), valid_f, scores)
    z = lax.axis_index(Z)
    shards = jnp.stack([(z * 2 + core) * n_y, (z * 2 + 1 - core) * n_y]) + y
    stats = shard_stats(gathered, unembed, other_unembed, shards * vocab_rows, n_y)
    plane = lax.all_to_all(stats, "y", 0, 0, tiled=True)
    plane = jnp.concatenate([merged(plane[:, 0:1]), jnp.sum(plane[:, 1:2], axis=0)])
    back = from_everyone(plane, Z)
    n_plane = lax.axis_size(PLANE)
    token_logp, token_loss, totals = finished(back, side, adv_rows, n_plane)
    totals = jnp.sum(lax.all_to_all(totals, PLANE, 0, 0, tiled=True), axis=(0, 1))
    loss = totals[0] / jnp.maximum(totals[1], 1.0)
    place = lax.axis_index("zl") * lax.axis_size("zh") + lax.axis_index("zh")
    first = place * local_rows
    return (
        lax.dynamic_slice_in_dim(token_logp, first, local_rows, 1),
        lax.dynamic_slice_in_dim(token_loss, first, local_rows, 1),
        lax.dynamic_slice_in_dim(adv_rows, first, 1, 1),
        loss,
    )


def solution(mesh):
    split = Mesh(
        mesh.devices.reshape(
            mesh.shape["prompt"] // 4, 2, 2, mesh.shape["sample"], mesh.shape["vocab"]
        ),
        ("zh", "zl", "c", "x", "y"),
    )
    in_specs = (
        P("x", ROW, None),
        P(ROW, None),
        P("x", ROW),
        P("x", ROW),
        P("x", ROW),
        P("x", ROW),
        P(PROMPT, "x"),
        P(PROMPT, "x"),
        P(PROMPT, "x"),
    )
    out_specs = (P("x", ROW), P("x", ROW), P(PROMPT, "x"), P())
    return jax.shard_map(local, mesh=split, in_specs=in_specs, out_specs=out_specs, check_vma=False)
```

```python
import jax
import jax.numpy as jnp
from jax import lax
from jax.experimental import pallas as pl
from jax.experimental.pallas import tpu as pltpu
from jax.sharding import Mesh
from jax.sharding import PartitionSpec as P


Z = ("zh", "zl")
ROW = ("zh", "zl", "c", "y")
PROMPT = ("zh", "zl", "c")
PLANE = ("c", "x", "y")
LANES = 128
FIELDS = 6
FULL_VMEM = 60 * 1024 * 2**10
KERNEL_VMEM = 48 * 2**20
LATE_VMEM = 24 * 2**20
SMALL_VMEM = 4 * 2**20

clip_low = 0.8
clip_high = 1.2
dual_clip = 3.0
kl_weight = 0.04
reward_unit = 0.01
std_floor = 0.5


def from_everyone(array, axis):
    devices = lax.axis_size(axis)
    return lax.all_to_all(
        jnp.broadcast_to(array[None], (devices, *array.shape)), axis, 0, 0, tiled=True
    )


def prep_kernel(y_ref, *refs):
    smalls, hidden_ref, out_ref, tall_ref = refs[:7], refs[7], refs[8], refs[9]
    landed, sems = refs[10:17], refs[17]
    copies = [
        pltpu.make_async_copy(src, dst, sems.at[i])
        for i, (src, dst) in enumerate(zip(smalls, landed))
    ]
    for copy in copies:
        copy.start()
    for copy in copies:
        copy.wait()
    ids_ref, old_ref, ref_ref, mask_ref, len_ref, valid_ref, reward_ref = landed
    local_rows, width = hidden_ref.shape[1:]
    blocks = width // LANES
    lane = lax.broadcasted_iota(jnp.int32, (local_rows, LANES), 1)
    line = lax.broadcasted_iota(jnp.int32, (local_rows, LANES), 0)
    field = lane // 3
    values = jnp.zeros((local_rows, LANES), jnp.float32)
    for r in range(local_rows):
        position = y_ref[0] * local_rows + r
        live = (mask_ref[0, r] == 1) & (position < len_ref[0]) & (valid_ref[0] == 1)
        whole = jnp.where(
            field == 0,
            ids_ref[0, r],
            jnp.where(
                field == 3,
                live.astype(jnp.int32),
                jnp.where(
                    field == 4, valid_ref[0], jnp.where(field == 5, reward_ref[0], 0)
                ),
            ),
        ).astype(jnp.float32)
        row = jnp.where(
            field == 1, old_ref[0, r], jnp.where(field == 2, ref_ref[0, r], whole)
        )
        values = jnp.where(line == r, row, values)
    first = values.astype(jnp.bfloat16).astype(jnp.float32)
    rest = values - first
    second = rest.astype(jnp.bfloat16).astype(jnp.float32)
    piece = lane - 3 * field
    side = jnp.where(piece == 0, first, jnp.where(piece == 1, second, rest - second))
    tall_ref[...] = jnp.zeros(tall_ref.shape, jnp.float32)
    for r in range(local_rows):
        at = r * (blocks + 1)
        for j in range(blocks):
            part = hidden_ref[0, r : r + 1, j * LANES : (j + 1) * LANES]
            tall_ref[at + j : at + j + 1, :] = part.astype(jnp.float32)
        tall_ref[at + blocks : at + blocks + 1, :] = side[r : r + 1, :]
    out_ref[...] = tall_ref[...].astype(jnp.bfloat16)


def prepared(y, smalls, hidden):
    _, local_rows, width = hidden.shape
    tall = -(-local_rows * (width // LANES + 1) // 8) * 8
    vmem = pl.BlockSpec(memory_space=pltpu.VMEM)
    return pl.pallas_call(
        prep_kernel,
        in_specs=[pl.BlockSpec(memory_space=pltpu.SMEM)]
        + [pl.BlockSpec(memory_space=pltpu.HBM)] * len(smalls)
        + [vmem],
        out_specs=vmem,
        out_shape=jax.ShapeDtypeStruct((tall, LANES), jnp.bfloat16),
        scratch_shapes=[
            pltpu.VMEM((tall, LANES), jnp.float32),
            *(pltpu.SMEM(small.shape, small.dtype) for small in smalls),
            pltpu.SemaphoreType.DMA((len(smalls),)),
        ],
        compiler_params=pltpu.CompilerParams(vmem_limit_bytes=FULL_VMEM),
        name="prep",
    )(y, *smalls, hidden)


def tail_kernel(back_ref, side_ref, adv_ref, logp_ref, loss_ref, totals_ref):
    lse = back_ref[:, 0, :]
    peak = jnp.max(lse, axis=0, keepdims=True)
    total = jnp.sum(jnp.exp(lse - peak), axis=0, keepdims=True)
    target = jnp.sum(back_ref[:, 1, :], axis=0, keepdims=True)
    raw_logp = target - (peak + jnp.log(total))
    live_float = side_ref[3:4, :]
    live = live_float > 0.5
    adv_rows = adv_ref[...]
    prob_ratio = jnp.exp(raw_logp - side_ref[1:2, :])
    gain_side = adv_rows * jnp.minimum(prob_ratio, clip_high)
    loss_side = jnp.maximum(adv_rows * jnp.maximum(prob_ratio, clip_low), dual_clip * adv_rows)
    objective = jnp.where(adv_rows >= 0.0, gain_side, loss_side)
    log_gap = side_ref[2:3, :] - raw_logp
    kl_term = jnp.exp(log_gap) - log_gap - 1.0
    token_loss = jnp.where(live, kl_weight * kl_term - objective, 0.0)
    logp_ref[...] = jnp.where(live, raw_logp, 0.0)
    loss_ref[...] = token_loss
    lane = lax.broadcasted_iota(jnp.int32, totals_ref.shape, 2)
    totals_ref[...] = jnp.where(
        lane == 0, jnp.sum(token_loss), jnp.where(lane == 1, jnp.sum(live_float), 0.0)
    )


def finished(back, side, adv_rows, devices):
    row = jax.ShapeDtypeStruct(adv_rows.shape, jnp.float32)
    vmem = pl.BlockSpec(memory_space=pltpu.VMEM)
    return pl.pallas_call(
        tail_kernel,
        in_specs=[vmem] * 3,
        out_specs=[vmem] * 3,
        out_shape=[row, row, jax.ShapeDtypeStruct((devices, 1, LANES), jnp.float32)],
        compiler_params=pltpu.CompilerParams(vmem_limit_bytes=SMALL_VMEM),
        name="tail",
    )(back, side, adv_rows)


CONTRACT = (((1,), (1,)), ((), ()))
FIRST = 64


def product(left, right):
    return lax.dot_general(left, right, CONTRACT, preferred_element_type=jnp.float32)


def row_ids(x_ref, width):
    pick = (lax.broadcasted_iota(jnp.int32, (8, LANES), 1) < 3).astype(jnp.bfloat16)
    return product(pick, x_ref[:, width:])[0:1].astype(jnp.int32)


def half_stats(logits, ids):
    peak = jnp.max(logits, axis=0, keepdims=True)
    total = jnp.sum(jnp.exp(logits - peak), axis=0, keepdims=True)
    hit = lax.broadcasted_iota(jnp.int32, logits.shape, 0) == ids
    return peak, total, jnp.sum(jnp.where(hit, logits, 0.0), axis=0, keepdims=True)


def joined(first, second):
    (peak_a, total_a, target_a), (peak_b, total_b, target_b) = first, second
    peak = jnp.maximum(peak_a, peak_b)
    total = total_a * jnp.exp(peak_a - peak) + total_b * jnp.exp(peak_b - peak)
    return jnp.concatenate([peak + jnp.log(total), target_a + target_b])


def early_kernel(
    scalars_ref, own_ref, other_ref, rows_ref, above_ref, below_ref, out_ref, x_ref, w_ref, sems
):
    per = out_ref.shape[2]
    width = own_ref.shape[1]
    cut = 8 * LANES
    copies = [
        pltpu.make_async_copy(own_ref.at[:, :cut], w_ref.at[0, :, :cut], sems.at[0]),
        pltpu.make_async_copy(own_ref.at[:, cut:], w_ref.at[0, :, cut:], sems.at[1]),
        pltpu.make_async_copy(other_ref, w_ref.at[1], sems.at[2]),
    ]
    for copy in copies:
        copy.start()
    x_ref[:per, :] = rows_ref[...]
    x_ref[per : 2 * per, :] = above_ref[...]
    x_ref[2 * per :, :] = below_ref[:FIRST, :]
    ids = row_ids(x_ref, width)
    copies[0].wait()
    logits = product(w_ref[0, :, :cut], x_ref[:, :cut])
    copies[1].wait()
    logits += product(w_ref[0, :, cut:], x_ref[:, cut:width])
    first = half_stats(logits, ids - scalars_ref[0])
    copies[2].wait()
    logits = product(w_ref[1], x_ref[:, :width])
    stats = joined(first, half_stats(logits, ids - scalars_ref[1]))
    out_ref[0] = stats[:, :per]
    out_ref[1] = stats[:, per : 2 * per]
    out_ref[2] = jnp.concatenate(
        [stats[:, 2 * per :], jnp.zeros((2, per - FIRST), jnp.float32)], axis=1
    )


def late_kernel(
    scalars_ref, own_ref, other_ref, below_ref, low_ref, high_ref, early_ref, out_ref, x_ref
):
    per = out_ref.shape[2]
    width = own_ref.shape[1]
    rest = per - FIRST
    half = per // 2
    x_ref[:rest, :] = below_ref[FIRST:, :]
    x_ref[rest : rest + half, :] = low_ref[...]
    x_ref[rest + half :, :] = high_ref[...]
    ids = row_ids(x_ref, width)
    first = half_stats(product(own_ref[...], x_ref[:, :width]), ids - scalars_ref[0])
    second = half_stats(product(other_ref[...], x_ref[:, :width]), ids - scalars_ref[1])
    stats = joined(first, second)
    y = scalars_ref[2]
    out_ref[y] = early_ref[0]
    out_ref[lax.rem(y + 1, 4)] = early_ref[1]
    out_ref[lax.rem(y + 3, 4)] = jnp.concatenate(
        [early_ref[2][:, :FIRST], stats[:, :rest]], axis=1
    )
    out_ref[lax.rem(y + 2, 4)] = stats[:, rest:]


def shard_stats(kernel, scalars, own, other, operands, groups, count, staged):
    vocab, width = own.shape
    per, full = operands[0].shape
    vmem = pl.BlockSpec(memory_space=pltpu.VMEM)
    weights = pl.BlockSpec(memory_space=pltpu.HBM) if staged else vmem
    scratch = [pltpu.VMEM((count, full), jnp.bfloat16)]
    if staged:
        scratch += [
            pltpu.VMEM((2, vocab, width), jnp.bfloat16),
            pltpu.SemaphoreType.DMA((3,)),
        ]
    return pl.pallas_call(
        kernel,
        in_specs=[pl.BlockSpec(memory_space=pltpu.SMEM), weights, weights]
        + [vmem] * len(operands),
        out_specs=vmem,
        out_shape=jax.ShapeDtypeStruct((groups, 2, per), jnp.float32),
        scratch_shapes=scratch,
        cost_estimate=pl.CostEstimate(
            flops=4 * count * width * vocab,
            bytes_accessed=2 * width * (count + 2 * vocab),
            transcendentals=2 * count * vocab,
        ),
        compiler_params=pltpu.CompilerParams(
            vmem_limit_bytes=KERNEL_VMEM if staged else LATE_VMEM
        ),
        name="early_stats" if staged else "late_stats",
    )(scalars, own, other, *operands)


def merged(lse):
    peak = jnp.max(lse, axis=0)
    return peak + jnp.log(jnp.sum(jnp.exp(lse - peak), axis=0))


def group_advantages(sums, valid_f, scores):
    group_count, first_moment, second_moment = (sums[i : i + 1] for i in range(3))
    safe_count = jnp.maximum(group_count, 1.0)
    group_mean = first_moment / safe_count
    spread = jnp.sqrt(jnp.maximum(second_moment / safe_count - group_mean * group_mean, 0.0))
    return valid_f * (scores - group_mean) / jnp.maximum(spread, std_floor)


def local(
    hidden, unembed, token_ids, old_logp, ref_logp, loss_mask, lengths, sample_valid, rewards
):
    _, local_rows, width = hidden.shape
    vocab_rows = unembed.shape[0]
    n_y = lax.axis_size("y")
    n_z = lax.axis_size(Z)
    column_rows = n_z * local_rows
    core = lax.axis_index("c")

    full = width + LANES
    y = lax.axis_index("y")
    singles = (lengths.reshape(1), sample_valid.reshape(1), rewards.reshape(1))
    smalls = (token_ids, old_logp, ref_logp, loss_mask, *singles)
    chunk = prepared(y.reshape(1), smalls, hidden)
    column = lax.all_gather(lax.all_gather(chunk, "zh", axis=0), "zl", axis=0)
    column = column.reshape(n_z, *chunk.shape)
    rows = column[:, : local_rows * full // LANES].reshape(column_rows, full)

    up = [(i, (i + 1) % n_y) for i in range(n_y)]
    down = [(i, (i - 1) % n_y) for i in range(n_y)]
    below = lax.ppermute(rows, "y", up)
    above = lax.ppermute(rows, "y", down)
    other_unembed = lax.ppermute(unembed, "c", [(0, 1), (1, 0)])
    half = column_rows // 2
    across_low = lax.ppermute(below[:half], "y", up)
    across_high = lax.ppermute(above[half:], "y", down)

    side = rows[:, width : width + 3 * FIELDS].astype(jnp.float32).T
    side = side.reshape(FIELDS, 3, column_rows)
    side = side[:, 0] + side[:, 1] + side[:, 2]
    valid_f = side[4:5]
    scores = side[5:6] * reward_unit
    moments = jnp.concatenate([valid_f, valid_f * scores, valid_f * scores * scores])
    terms = from_everyone(moments, "x")
    adv_rows = group_advantages(jnp.sum(terms, axis=0), valid_f, scores)
    z = lax.axis_index(Z)
    scalars = jnp.stack(
        [
            ((z * 2 + core) * n_y + y) * vocab_rows,
            ((z * 2 + 1 - core) * n_y + y) * vocab_rows,
            y,
        ]
    )
    stats = shard_stats(
        early_kernel, scalars, unembed, other_unembed, [rows, above, below], 3,
        2 * column_rows + FIRST, True,
    )
    stats = shard_stats(
        late_kernel, scalars, unembed, other_unembed, [below, across_low, across_high, stats],
        n_y, 2 * column_rows - FIRST, False,
    )
    plane = lax.all_to_all(stats, "y", 0, 0, tiled=True)
    plane = jnp.concatenate([merged(plane[:, 0:1]), jnp.sum(plane[:, 1:2], axis=0)])
    back = from_everyone(plane, Z)
    n_plane = lax.axis_size(PLANE)
    token_logp, token_loss, totals = finished(back, side, adv_rows, n_plane)
    totals = jnp.sum(lax.all_to_all(totals, PLANE, 0, 0, tiled=True), axis=(0, 1))
    loss = totals[0] / jnp.maximum(totals[1], 1.0)
    place = lax.axis_index("zl") * lax.axis_size("zh") + lax.axis_index("zh")
    first = place * local_rows
    return (
        lax.dynamic_slice_in_dim(token_logp, first, local_rows, 1),
        lax.dynamic_slice_in_dim(token_loss, first, local_rows, 1),
        lax.dynamic_slice_in_dim(adv_rows, first, 1, 1),
        loss,
    )


def solution(mesh):
    split = Mesh(
        mesh.devices.reshape(
            mesh.shape["prompt"] // 4, 2, 2, mesh.shape["sample"], mesh.shape["vocab"]
        ),
        ("zh", "zl", "c", "x", "y"),
    )
    in_specs = (
        P("x", ROW, None),
        P(ROW, None),
        P("x", ROW),
        P("x", ROW),
        P("x", ROW),
        P("x", ROW),
        P(PROMPT, "x"),
        P(PROMPT, "x"),
        P(PROMPT, "x"),
    )
    out_specs = (P("x", ROW), P("x", ROW), P(PROMPT, "x"), P())
    return jax.shard_map(
        local, mesh=split, in_specs=in_specs, out_specs=out_specs, check_vma=False
    )
```

```python
import jax
import jax.numpy as jnp
from jax import lax
from jax.experimental import pallas as pl
from jax.experimental.pallas import tpu as pltpu
from jax.sharding import Mesh
from jax.sharding import PartitionSpec as P


Z = ("zh", "zl")
ROW = ("zh", "zl", "c", "y")
PROMPT = ("zh", "zl", "c")
PLANE = ("c", "x", "y")
LANES = 128
FIELDS = 6
FULL_VMEM = 60 * 1024 * 2**10
KERNEL_VMEM = 48 * 2**20
LATE_VMEM = 24 * 2**20
SMALL_VMEM = 4 * 2**20

clip_low = 0.8
clip_high = 1.2
dual_clip = 3.0
kl_weight = 0.04
reward_unit = 0.01
std_floor = 0.5


def from_everyone(array, axis):
    devices = lax.axis_size(axis)
    return lax.all_to_all(
        jnp.broadcast_to(array[None], (devices, *array.shape)), axis, 0, 0, tiled=True
    )


def prep_kernel(y_ref, *refs):
    smalls, hidden_src, out_ref, tall_ref, hidden_ref = refs[:7], *refs[7:11]
    landed, sems = refs[11:18], refs[18]
    copies = [
        pltpu.make_async_copy(src, dst, sems.at[i])
        for i, (src, dst) in enumerate(zip((*smalls, hidden_src), (*landed, hidden_ref)))
    ]
    for copy in copies:
        copy.start()
    tall_ref[...] = jnp.zeros(tall_ref.shape, jnp.float32)
    for copy in copies:
        copy.wait()
    ids_ref, old_ref, ref_ref, mask_ref, len_ref, valid_ref, reward_ref = landed
    local_rows, width = hidden_ref.shape[1:]
    blocks = width // LANES
    lane = lax.broadcasted_iota(jnp.int32, (local_rows, LANES), 1)
    line = lax.broadcasted_iota(jnp.int32, (local_rows, LANES), 0)
    field = lane // 3
    values = jnp.zeros((local_rows, LANES), jnp.float32)
    for r in range(local_rows):
        position = y_ref[0] * local_rows + r
        live = (mask_ref[0, r] == 1) & (position < len_ref[0]) & (valid_ref[0] == 1)
        whole = jnp.where(
            field == 0,
            ids_ref[0, r],
            jnp.where(
                field == 3,
                live.astype(jnp.int32),
                jnp.where(
                    field == 4, valid_ref[0], jnp.where(field == 5, reward_ref[0], 0)
                ),
            ),
        ).astype(jnp.float32)
        row = jnp.where(
            field == 1, old_ref[0, r], jnp.where(field == 2, ref_ref[0, r], whole)
        )
        values = jnp.where(line == r, row, values)
    first = values.astype(jnp.bfloat16).astype(jnp.float32)
    rest = values - first
    second = rest.astype(jnp.bfloat16).astype(jnp.float32)
    piece = lane - 3 * field
    side = jnp.where(piece == 0, first, jnp.where(piece == 1, second, rest - second))
    for r in range(local_rows):
        at = r * (blocks + 1)
        for j in range(blocks):
            part = hidden_ref[0, r : r + 1, j * LANES : (j + 1) * LANES]
            tall_ref[at + j : at + j + 1, :] = part.astype(jnp.float32)
        tall_ref[at + blocks : at + blocks + 1, :] = side[r : r + 1, :]
    out_ref[...] = tall_ref[...].astype(jnp.bfloat16)


def prepared(y, smalls, hidden):
    _, local_rows, width = hidden.shape
    tall = -(-local_rows * (width // LANES + 1) // 8) * 8
    vmem = pl.BlockSpec(memory_space=pltpu.VMEM)
    return pl.pallas_call(
        prep_kernel,
        in_specs=[pl.BlockSpec(memory_space=pltpu.SMEM)]
        + [pl.BlockSpec(memory_space=pltpu.HBM)] * (len(smalls) + 1),
        out_specs=vmem,
        out_shape=jax.ShapeDtypeStruct((tall, LANES), jnp.bfloat16),
        scratch_shapes=[
            pltpu.VMEM((tall, LANES), jnp.float32),
            pltpu.VMEM(hidden.shape, hidden.dtype),
            *(pltpu.SMEM(small.shape, small.dtype) for small in smalls),
            pltpu.SemaphoreType.DMA((len(smalls) + 1,)),
        ],
        compiler_params=pltpu.CompilerParams(vmem_limit_bytes=FULL_VMEM),
        name="prep",
    )(y, *smalls, hidden)


def tail_kernel(back_ref, side_ref, adv_ref, logp_ref, loss_ref, totals_ref):
    lse = back_ref[:, 0, :]
    peak = jnp.max(lse, axis=0, keepdims=True)
    total = jnp.sum(jnp.exp(lse - peak), axis=0, keepdims=True)
    target = jnp.sum(back_ref[:, 1, :], axis=0, keepdims=True)
    raw_logp = target - (peak + jnp.log(total))
    live_float = side_ref[3:4, :]
    live = live_float > 0.5
    adv_rows = adv_ref[...]
    prob_ratio = jnp.exp(raw_logp - side_ref[1:2, :])
    gain_side = adv_rows * jnp.minimum(prob_ratio, clip_high)
    loss_side = jnp.maximum(adv_rows * jnp.maximum(prob_ratio, clip_low), dual_clip * adv_rows)
    objective = jnp.where(adv_rows >= 0.0, gain_side, loss_side)
    log_gap = side_ref[2:3, :] - raw_logp
    kl_term = jnp.exp(log_gap) - log_gap - 1.0
    token_loss = jnp.where(live, kl_weight * kl_term - objective, 0.0)
    logp_ref[...] = jnp.where(live, raw_logp, 0.0)
    loss_ref[...] = token_loss
    lane = lax.broadcasted_iota(jnp.int32, totals_ref.shape, 2)
    totals_ref[...] = jnp.where(
        lane == 0, jnp.sum(token_loss), jnp.where(lane == 1, jnp.sum(live_float), 0.0)
    )


def finished(back, side, adv_rows, devices):
    row = jax.ShapeDtypeStruct(adv_rows.shape, jnp.float32)
    vmem = pl.BlockSpec(memory_space=pltpu.VMEM)
    return pl.pallas_call(
        tail_kernel,
        in_specs=[vmem] * 3,
        out_specs=[vmem] * 3,
        out_shape=[row, row, jax.ShapeDtypeStruct((devices, 1, LANES), jnp.float32)],
        compiler_params=pltpu.CompilerParams(vmem_limit_bytes=SMALL_VMEM),
        name="tail",
    )(back, side, adv_rows)


CONTRACT = (((1,), (1,)), ((), ()))
FIRST = 64


def product(left, right):
    return lax.dot_general(left, right, CONTRACT, preferred_element_type=jnp.float32)


def row_ids(x_ref, width):
    pick = (lax.broadcasted_iota(jnp.int32, (8, LANES), 1) < 3).astype(jnp.bfloat16)
    return product(pick, x_ref[:, width:])[0:1].astype(jnp.int32)


def half_stats(logits, ids):
    peak = jnp.max(logits, axis=0, keepdims=True)
    total = jnp.sum(jnp.exp(logits - peak), axis=0, keepdims=True)
    hit = lax.broadcasted_iota(jnp.int32, logits.shape, 0) == ids
    return peak, total, jnp.sum(jnp.where(hit, logits, 0.0), axis=0, keepdims=True)


def joined(first, second):
    (peak_a, total_a, target_a), (peak_b, total_b, target_b) = first, second
    peak = jnp.maximum(peak_a, peak_b)
    total = total_a * jnp.exp(peak_a - peak) + total_b * jnp.exp(peak_b - peak)
    return jnp.concatenate([peak + jnp.log(total), target_a + target_b])


def early_kernel(
    scalars_ref, own_ref, other_ref, rows_ref, above_ref, below_ref, out_ref, x_ref, w_ref, sems
):
    per = out_ref.shape[2]
    width = own_ref.shape[1]
    cut = 8 * LANES
    copies = [
        pltpu.make_async_copy(own_ref.at[:, :cut], w_ref.at[0, :, :cut], sems.at[0]),
        pltpu.make_async_copy(own_ref.at[:, cut:], w_ref.at[0, :, cut:], sems.at[1]),
        pltpu.make_async_copy(other_ref, w_ref.at[1], sems.at[2]),
    ]
    for copy in copies:
        copy.start()
    x_ref[:per, :] = rows_ref[...]
    x_ref[per : 2 * per, :] = above_ref[...]
    x_ref[2 * per :, :] = below_ref[:FIRST, :]
    ids = row_ids(x_ref, width)
    copies[0].wait()
    logits = product(w_ref[0, :, :cut], x_ref[:, :cut])
    copies[1].wait()
    logits += product(w_ref[0, :, cut:], x_ref[:, cut:width])
    first = half_stats(logits, ids - scalars_ref[0])
    copies[2].wait()
    logits = product(w_ref[1], x_ref[:, :width])
    stats = joined(first, half_stats(logits, ids - scalars_ref[1]))
    out_ref[0] = stats[:, :per]
    out_ref[1] = stats[:, per : 2 * per]
    out_ref[2] = jnp.concatenate(
        [stats[:, 2 * per :], jnp.zeros((2, per - FIRST), jnp.float32)], axis=1
    )


def late_kernel(
    scalars_ref, own_ref, other_ref, below_ref, low_ref, high_ref, early_ref, out_ref, x_ref
):
    per = out_ref.shape[2]
    width = own_ref.shape[1]
    rest = per - FIRST
    half = per // 2
    x_ref[:rest, :] = below_ref[FIRST:, :]
    x_ref[rest : rest + half, :] = low_ref[...]
    x_ref[rest + half :, :] = high_ref[...]
    ids = row_ids(x_ref, width)
    first = half_stats(product(own_ref[...], x_ref[:, :width]), ids - scalars_ref[0])
    second = half_stats(product(other_ref[...], x_ref[:, :width]), ids - scalars_ref[1])
    stats = joined(first, second)
    y = scalars_ref[2]
    out_ref[y] = early_ref[0]
    out_ref[lax.rem(y + 1, 4)] = early_ref[1]
    out_ref[lax.rem(y + 3, 4)] = jnp.concatenate(
        [early_ref[2][:, :FIRST], stats[:, :rest]], axis=1
    )
    out_ref[lax.rem(y + 2, 4)] = stats[:, rest:]


def shard_stats(kernel, scalars, own, other, operands, groups, count, staged):
    vocab, width = own.shape
    per, full = operands[0].shape
    vmem = pl.BlockSpec(memory_space=pltpu.VMEM)
    weights = pl.BlockSpec(memory_space=pltpu.HBM) if staged else vmem
    scratch = [pltpu.VMEM((count, full), jnp.bfloat16)]
    if staged:
        scratch += [
            pltpu.VMEM((2, vocab, width), jnp.bfloat16),
            pltpu.SemaphoreType.DMA((3,)),
        ]
    return pl.pallas_call(
        kernel,
        in_specs=[pl.BlockSpec(memory_space=pltpu.SMEM), weights, weights]
        + [vmem] * len(operands),
        out_specs=vmem,
        out_shape=jax.ShapeDtypeStruct((groups, 2, per), jnp.float32),
        scratch_shapes=scratch,
        cost_estimate=pl.CostEstimate(
            flops=4 * count * width * vocab,
            bytes_accessed=2 * width * (count + 2 * vocab),
            transcendentals=2 * count * vocab,
        ),
        compiler_params=pltpu.CompilerParams(
            vmem_limit_bytes=KERNEL_VMEM if staged else LATE_VMEM
        ),
        name="early_stats" if staged else "late_stats",
    )(scalars, own, other, *operands)


def merged(lse):
    peak = jnp.max(lse, axis=0)
    return peak + jnp.log(jnp.sum(jnp.exp(lse - peak), axis=0))


def group_advantages(sums, valid_f, scores):
    group_count, first_moment, second_moment = (sums[i : i + 1] for i in range(3))
    safe_count = jnp.maximum(group_count, 1.0)
    group_mean = first_moment / safe_count
    spread = jnp.sqrt(jnp.maximum(second_moment / safe_count - group_mean * group_mean, 0.0))
    return valid_f * (scores - group_mean) / jnp.maximum(spread, std_floor)


def local(
    hidden, unembed, token_ids, old_logp, ref_logp, loss_mask, lengths, sample_valid, rewards
):
    _, local_rows, width = hidden.shape
    vocab_rows = unembed.shape[0]
    n_y = lax.axis_size("y")
    n_z = lax.axis_size(Z)
    column_rows = n_z * local_rows
    core = lax.axis_index("c")

    full = width + LANES
    y = lax.axis_index("y")
    singles = (lengths.reshape(1), sample_valid.reshape(1), rewards.reshape(1))
    smalls = (token_ids, old_logp, ref_logp, loss_mask, *singles)
    chunk = prepared(y.reshape(1), smalls, hidden)
    column = lax.all_gather(lax.all_gather(chunk, "zh", axis=0), "zl", axis=0)
    column = column.reshape(n_z, *chunk.shape)
    rows = column[:, : local_rows * full // LANES].reshape(column_rows, full)

    up = [(i, (i + 1) % n_y) for i in range(n_y)]
    down = [(i, (i - 1) % n_y) for i in range(n_y)]
    below = lax.ppermute(rows, "y", up)
    above = lax.ppermute(rows, "y", down)
    other_unembed = lax.ppermute(unembed, "c", [(0, 1), (1, 0)])
    half = column_rows // 2
    across_low = lax.ppermute(below[:half], "y", up)
    across_high = lax.ppermute(above[half:], "y", down)

    side = rows[:, width : width + 3 * FIELDS].astype(jnp.float32).T
    side = side.reshape(FIELDS, 3, column_rows)
    side = side[:, 0] + side[:, 1] + side[:, 2]
    valid_f = side[4:5]
    scores = side[5:6] * reward_unit
    moments = jnp.concatenate([valid_f, valid_f * scores, valid_f * scores * scores])
    terms = from_everyone(moments, "x")
    adv_rows = group_advantages(jnp.sum(terms, axis=0), valid_f, scores)
    z = lax.axis_index(Z)
    scalars = jnp.stack(
        [
            ((z * 2 + core) * n_y + y) * vocab_rows,
            ((z * 2 + 1 - core) * n_y + y) * vocab_rows,
            y,
        ]
    )
    stats = shard_stats(
        early_kernel, scalars, unembed, other_unembed, [rows, above, below], 3,
        2 * column_rows + FIRST, True,
    )
    stats = shard_stats(
        late_kernel, scalars, unembed, other_unembed, [below, across_low, across_high, stats],
        n_y, 2 * column_rows - FIRST, False,
    )
    plane = lax.all_to_all(stats, "y", 0, 0, tiled=True)
    plane = jnp.concatenate([merged(plane[:, 0:1]), jnp.sum(plane[:, 1:2], axis=0)])
    back = from_everyone(plane, Z)
    n_plane = lax.axis_size(PLANE)
    token_logp, token_loss, totals = finished(back, side, adv_rows, n_plane)
    totals = jnp.sum(lax.all_to_all(totals, PLANE, 0, 0, tiled=True), axis=(0, 1))
    loss = totals[0] / jnp.maximum(totals[1], 1.0)
    place = lax.axis_index("zl") * lax.axis_size("zh") + lax.axis_index("zh")
    first = place * local_rows
    return (
        lax.dynamic_slice_in_dim(token_logp, first, local_rows, 1),
        lax.dynamic_slice_in_dim(token_loss, first, local_rows, 1),
        lax.dynamic_slice_in_dim(adv_rows, first, 1, 1),
        loss,
    )


def solution(mesh):
    split = Mesh(
        mesh.devices.reshape(
            mesh.shape["prompt"] // 4, 2, 2, mesh.shape["sample"], mesh.shape["vocab"]
        ),
        ("zh", "zl", "c", "x", "y"),
    )
    in_specs = (
        P("x", ROW, None),
        P(ROW, None),
        P("x", ROW),
        P("x", ROW),
        P("x", ROW),
        P("x", ROW),
        P(PROMPT, "x"),
        P(PROMPT, "x"),
        P(PROMPT, "x"),
    )
    out_specs = (P("x", ROW), P("x", ROW), P(PROMPT, "x"), P())
    return jax.shard_map(
        local, mesh=split, in_specs=in_specs, out_specs=out_specs, check_vma=False
    )
```
